32 devices in a mesh: dp: 1 (over z), ctx: 32 (over y, x, core).
Axes of the slice: x: 4, y: 4, z: 1, core: 2. Of those that a mesh axis runs over, the one named last changes fastest.
The devices are a block of a 4x4x8 slice.
Arguments:
- x_chunk: bfloat16 [16384, 640], P(('dp', 'ctx'))
- cache_len: int32 [1], P('dp')
- k_cache: bfloat16 [2, 16384, 1, 256], P(None, ('dp', 'ctx'))
- v_cache: bfloat16 [2, 16384, 1, 256], P(None, ('dp', 'ctx'))
- k_local: bfloat16 [2, 512, 1, 256], P(None, 'dp')
- v_local: bfloat16 [2, 512, 1, 256], P(None, 'dp')
- g_attn: bfloat16 [4, 640], replicated
- g_mlp: bfloat16 [4, 640], replicated
- w_q: bfloat16 [4, 640, 1024], replicated
- w_k: bfloat16 [4, 640, 256], replicated
- w_v: bfloat16 [4, 640, 256], replicated
- w_o: bfloat16 [4, 1024, 640], replicated
- w_gate: bfloat16 [4, 640, 2048], replicated
- w_up: bfloat16 [4, 640, 2048], replicated
- w_down: bfloat16 [4, 2048, 640], replicated
Outputs:
- output: bfloat16 [16384, 640], P(('dp', 'ctx'))
All inputs are finite; a program needn't handle non-finite values.
Results may differ from the reference program's by a relative error of at most 0.02.
Values are sent between devices in bfloat16 or wider.
A program may use at most 768 MiB of HBM per device.

```python
import math
import jax
import jax.numpy as jnp
from jax import lax

D_MODEL = 640
NUM_HEADS = 4
KV_HEADS = 1
HEAD_DIM = 256
WINDOW = 512
FF_DIM = 2048
SEQ_NEW = 16384
CACHE_SIZE = 16384
QUERY_ROWS = 128
NUM_PAIRS = 2
NORM_EPS = 1e-6


def draw_normal(rng_key, arr_shape, factor):
    return jax.random.normal(rng_key, arr_shape, jnp.float32) * factor


def setup_inputs(seed: int = 0, part: int = 0) -> dict:
    part_keys = jax.random.split(jax.random.fold_in(jax.random.key(seed), part), 6)
    shared_keys = jax.random.split(jax.random.key(seed + 1), 9)
    n_layers = 2 * NUM_PAIRS
    q_width = NUM_HEADS * HEAD_DIM
    kv_width = KV_HEADS * HEAD_DIM
    gain_local = math.log(max(WINDOW / 8.0, 2.0)) ** 0.25
    gain_global = math.log(max((CACHE_SIZE + SEQ_NEW) / 16.0, 2.0)) ** 0.25
    gain_base = jnp.tile(jnp.array([gain_local, gain_global], jnp.float32), NUM_PAIRS)
    cache_shape = (NUM_PAIRS, CACHE_SIZE, KV_HEADS, HEAD_DIM)
    local_shape = (NUM_PAIRS, WINDOW, KV_HEADS, HEAD_DIM)
    x_chunk = draw_normal(part_keys[0], (SEQ_NEW, D_MODEL), 1.0).astype(jnp.bfloat16)
    cache_len = jax.random.randint(part_keys[1], (1,), CACHE_SIZE // 2, CACHE_SIZE + 1, jnp.int32)
    k_cache = draw_normal(part_keys[2], cache_shape, gain_global).astype(jnp.bfloat16)
    v_cache = draw_normal(part_keys[3], cache_shape, gain_global).astype(jnp.bfloat16)
    k_local = draw_normal(part_keys[4], local_shape, gain_local).astype(jnp.bfloat16)
    v_local = draw_normal(part_keys[5], local_shape, gain_local).astype(jnp.bfloat16)
    g_attn = (gain_base[:, None] * (1.0 + draw_normal(shared_keys[0], (n_layers, D_MODEL), 0.2))).astype(jnp.bfloat16)
    g_mlp = (1.0 + draw_normal(shared_keys[1], (n_layers, D_MODEL), 0.2)).astype(jnp.bfloat16)
    w_q = draw_normal(shared_keys[2], (n_layers, D_MODEL, q_width), D_MODEL ** -0.5).astype(jnp.bfloat16)
    w_k = draw_normal(shared_keys[3], (n_layers, D_MODEL, kv_width), D_MODEL ** -0.5).astype(jnp.bfloat16)
    w_v = draw_normal(shared_keys[4], (n_layers, D_MODEL, kv_width), D_MODEL ** -0.5).astype(jnp.bfloat16)
    w_o = draw_normal(shared_keys[5], (n_layers, q_width, D_MODEL), q_width ** -0.5).astype(jnp.bfloat16)
    w_gate = draw_normal(shared_keys[6], (n_layers, D_MODEL, FF_DIM), D_MODEL ** -0.5).astype(jnp.bfloat16)
    w_up = draw_normal(shared_keys[7], (n_layers, D_MODEL, FF_DIM), D_MODEL ** -0.5).astype(jnp.bfloat16)
    w_down = draw_normal(shared_keys[8], (n_layers, FF_DIM, D_MODEL), FF_DIM ** -0.5).astype(jnp.bfloat16)
    return {'x_chunk': x_chunk, 'cache_len': cache_len, 'k_cache': k_cache, 'v_cache': v_cache,
            'k_local': k_local, 'v_local': v_local, 'g_attn': g_attn, 'g_mlp': g_mlp,
            'w_q': w_q, 'w_k': w_k, 'w_v': w_v, 'w_o': w_o,
            'w_gate': w_gate, 'w_up': w_up, 'w_down': w_down}


def rms_norm(rows_in, gain_vec):
    rows_f32 = rows_in.astype(jnp.float32)
    inv_rms = lax.rsqrt(jnp.mean(rows_f32 * rows_f32, axis=-1, keepdims=True) + NORM_EPS)
    return (rows_f32 * inv_rms * gain_vec.astype(jnp.float32)).astype(jnp.bfloat16)


def project(rows_in, weight):
    return jnp.dot(rows_in, weight, preferred_element_type=jnp.float32).astype(jnp.bfloat16)


def qkv_heads(normed, w_query, w_key, w_value):
    groups = NUM_HEADS // KV_HEADS
    queries = project(normed, w_query).reshape(SEQ_NEW, KV_HEADS, groups, HEAD_DIM)
    new_k = project(normed, w_key).reshape(SEQ_NEW, KV_HEADS, HEAD_DIM)
    new_v = project(normed, w_value).reshape(SEQ_NEW, KV_HEADS, HEAD_DIM)
    return queries, new_k, new_v


def attend(score_list, value_list):
    row_max = score_list[0].max(axis=-1)
    for part_scores in score_list[1:]:
        row_max = jnp.maximum(row_max, part_scores.max(axis=-1))
    row_sum = 0.0
    weighted = 0.0
    for part_scores, part_values in zip(score_list, value_list):
        part_probs = jnp.exp(part_scores - row_max[..., None])
        row_sum = row_sum + part_probs.sum(axis=-1)
        weighted = weighted + jnp.einsum('hgqk,khd->qhgd', part_probs.astype(jnp.bfloat16).astype(jnp.float32), part_values.astype(jnp.float32))
    return (weighted / jnp.transpose(row_sum, (2, 0, 1))[..., None]).astype(jnp.bfloat16)


def local_attention(queries, ext_k, ext_v):
    score_scale = HEAD_DIM ** -0.5
    rel_pos = jnp.arange(WINDOW + QUERY_ROWS)[None, :] - jnp.arange(QUERY_ROWS)[:, None]
    band_mask = (rel_pos > 0) & (rel_pos <= WINDOW)

    def one_block(block_idx):
        row_start = block_idx * QUERY_ROWS
        q_rows = lax.dynamic_slice_in_dim(queries, row_start, QUERY_ROWS, axis=0).astype(jnp.float32)
        k_rows = lax.dynamic_slice_in_dim(ext_k, row_start, WINDOW + QUERY_ROWS, axis=0)
        v_rows = lax.dynamic_slice_in_dim(ext_v, row_start, WINDOW + QUERY_ROWS, axis=0)
        scores = jnp.einsum('qhgd,khd->hgqk', q_rows, k_rows.astype(jnp.float32)) * score_scale
        scores = jnp.where(band_mask, scores, -jnp.inf)
        return attend([scores], [v_rows])

    blocks = lax.map(one_block, jnp.arange(SEQ_NEW // QUERY_ROWS))
    return blocks.reshape(SEQ_NEW, NUM_HEADS * HEAD_DIM)


def global_attention(queries, cache_k, cache_v, new_k, new_v, valid_len):
    score_scale = HEAD_DIM ** -0.5
    cache_mask = jnp.arange(CACHE_SIZE) < valid_len
    new_pos = jnp.arange(SEQ_NEW)
    cache_f32 = cache_k.astype(jnp.float32)
    new_f32 = new_k.astype(jnp.float32)

    def one_block(block_idx):
        row_start = block_idx * QUERY_ROWS
        q_rows = lax.dynamic_slice_in_dim(queries, row_start, QUERY_ROWS, axis=0).astype(jnp.float32)
        q_pos = row_start + jnp.arange(QUERY_ROWS)
        cache_scores = jnp.einsum('qhgd,khd->hgqk', q_rows, cache_f32) * score_scale
        cache_scores = jnp.where(cache_mask, cache_scores, -jnp.inf)
        new_scores = jnp.einsum('qhgd,khd->hgqk', q_rows, new_f32) * score_scale
        new_scores = jnp.where(new_pos[None, :] <= q_pos[:, None], new_scores, -jnp.inf)
        return attend([cache_scores, new_scores], [cache_v, new_v])

    blocks = lax.map(one_block, jnp.arange(SEQ_NEW // QUERY_ROWS))
    return blocks.reshape(SEQ_NEW, NUM_HEADS * HEAD_DIM)


def add_residual(hidden, attn_out, w_out):
    return (hidden.astype(jnp.float32) + jnp.dot(attn_out, w_out, preferred_element_type=jnp.float32)).astype(jnp.bfloat16)


def mlp_block(hidden, gain_vec, w_gate, w_up, w_down):
    normed = rms_norm(hidden, gain_vec)
    gate_pre = jnp.dot(normed, w_gate, preferred_element_type=jnp.float32)
    up_pre = jnp.dot(normed, w_up, preferred_element_type=jnp.float32)
    act_bf16 = (jax.nn.gelu(gate_pre, approximate=True) * up_pre).astype(jnp.bfloat16)
    return (hidden.astype(jnp.float32) + jnp.dot(act_bf16, w_down, preferred_element_type=jnp.float32)).astype(jnp.bfloat16)


def reference(x_chunk, cache_len, k_cache, v_cache, k_local, v_local, g_attn, g_mlp, w_q, w_k, w_v, w_o, w_gate, w_up, w_down):
    hidden = x_chunk
    for pair_idx in range(NUM_PAIRS):
        layer_idx = 2 * pair_idx
        queries, new_k, new_v = qkv_heads(rms_norm(hidden, g_attn[layer_idx]), w_q[layer_idx], w_k[layer_idx], w_v[layer_idx])
        ext_k = jnp.concatenate([k_local[pair_idx], new_k], axis=0)
        ext_v = jnp.concatenate([v_local[pair_idx], new_v], axis=0)
        attn_out = local_attention(queries, ext_k, ext_v)
        hidden = add_residual(hidden, attn_out, w_o[layer_idx])
        hidden = mlp_block(hidden, g_mlp[layer_idx], w_gate[layer_idx], w_up[layer_idx], w_down[layer_idx])
        layer_idx = 2 * pair_idx + 1
        queries, new_k, new_v = qkv_heads(rms_norm(hidden, g_attn[layer_idx]), w_q[layer_idx], w_k[layer_idx], w_v[layer_idx])
        attn_out = global_attention(queries, k_cache[pair_idx], v_cache[pair_idx], new_k, new_v, cache_len[0])
        hidden = add_residual(hidden, attn_out, w_o[layer_idx])
        hidden = mlp_block(hidden, g_mlp[layer_idx], w_gate[layer_idx], w_up[layer_idx], w_down[layer_idx])
    return hidden
```

```python
import functools
import jax, jax.numpy as jnp
from jax import lax
from jax.experimental import pallas as pl
from jax.experimental.pallas import tpu as pltpu
from jax.sharding import PartitionSpec as P

NORM_EPS = 1e-6
BAND_ROWS = 256
FLASH_ROWS = 256

LOG2E = 1.4426950408889634

def flash_unit(q, kt_list, v_list, m_ref, l_ref, acc_ref, rows, head, scale2, lim=None):
    lanes = pl.ds(pl.multiple_of(head * 128, 128), 128)
    hd = q.shape[1]
    s_list = [jnp.dot(q, kt, preferred_element_type=jnp.float32) for kt in kt_list]
    if lim is not None:
        col = lax.broadcasted_iota(jnp.int32, s_list[0].shape, 1)
        s_list = [jnp.where(col < lim, s, -jnp.inf) for s in s_list]
    parts = [s[:, i:i + 128] for s in s_list for i in range(0, s.shape[1], 128)]
    mx = parts[0]
    for part in parts[1:]:
        mx = jnp.maximum(mx, part)
    m_old = m_ref[rows, lanes]
    m_new = jnp.maximum(m_old, jnp.max(mx, axis=1, keepdims=True))
    alpha = jnp.exp2((m_old - m_new) * scale2)
    probs = [jnp.exp2((part - m_new) * scale2) for part in parts]
    total = probs[0]
    for prob in probs[1:]:
        total = total + prob
    m_ref[rows, lanes] = m_new
    l_ref[rows, lanes] = l_ref[rows, lanes] * alpha + total
    per = kt_list[0].shape[1] // 128
    pv = None
    for idx, v in enumerate(v_list):
        p = jnp.concatenate([x.astype(jnp.bfloat16) for x in probs[idx * per:(idx + 1) * per]], axis=1)
        term = jnp.dot(p, v, preferred_element_type=jnp.float32)
        pv = term if pv is None else pv + term
    cols = pl.ds(pl.multiple_of(head * hd, hd), hd)
    acc_ref[rows, cols] = acc_ref[rows, cols] * jnp.concatenate([alpha] * (hd // 128), axis=1) + pv


def plan(len_ref, mode, n, size):
    dev = lax.axis_index('ctx')
    par = lax.rem(dev, 2)
    if mode == 'cache':
        length = len_ref[0]
        pairs = length // (2 * size)
        rest = jnp.clip(length - pairs * (2 * size) - size * par, 0, size)
        n_full = pairs + rest // size
        return 0, n_full, n_full, rest - rest // size * size
    even_chunk = jnp.where(par == 0, dev, dev - 1)
    odd_chunk = jnp.where(par == 0, n - dev - 1, n - dev)
    q_chunk = jnp.where(par == 0, even_chunk, odd_chunk) if mode == 'own' else jnp.where(par == 0, odd_chunk, even_chunk)
    count = (q_chunk + 1 - par) // 2
    start = jnp.where(par == 0, 0, n // 2 - count)
    tail = jnp.where(par == 0, count, n // 2 - count - 1)
    return start, count, tail, jnp.where(lax.rem(q_chunk, 2) == par, 1, 0)


def flash_kernel(len_ref, q_ref, kt_hbm, v_hbm, acc_in, m_in, l_in, acc_ref, m_ref, l_ref, kbuf, vbuf, sems, *, bm, mode, heads, n):
    first = mode == 'cache'
    n_rows = q_ref.shape[0]
    hd = q_ref.shape[1] // heads
    ck = kt_hbm.shape[2]
    scale2 = LOG2E * hd ** -0.5
    start, n_full, tail, limit = plan(len_ref, mode, n, ck)
    n_two = n_full // 2
    odd = n_full - 2 * n_two

    def copies(slot, chunk, count):
        for i in range(count):
            yield pltpu.make_async_copy(kt_hbm.at[chunk + i], kbuf.at[slot, i], sems.at[slot, 2 * i])
            yield pltpu.make_async_copy(v_hbm.at[chunk + i], vbuf.at[slot, i], sems.at[slot, 2 * i + 1])

    @pl.when(n_two > 0)
    def _():
        for cp in copies(0, start, 2): cp.start()
    @pl.when(odd > 0)
    def _():
        for cp in copies(2, start + 2 * n_two, 1): cp.start()
    @pl.when(limit > 0)
    def _():
        for cp in copies(3, tail, 1): cp.start()
    if first:
        m_ref[...] = jnp.full_like(m_ref, -jnp.inf)
        l_ref[...] = jnp.zeros_like(l_ref)
        acc_ref[...] = jnp.zeros_like(acc_ref)
    else:
        m_ref[...] = m_in[...]
        l_ref[...] = l_in[...]
        acc_ref[...] = acc_in[...]

    def unit(slot, count, masked, head, r0):
        rows = pl.ds(r0, bm)
        q = q_ref[rows, pl.ds(pl.multiple_of(head * hd, hd), hd)]
        lim = None
        if masked:
            lim = limit if first else lax.broadcasted_iota(jnp.int32, (bm, 1), 0) + (r0 + 1)
        flash_unit(q, [kbuf[slot, i] for i in range(count)], [vbuf[slot, i] for i in range(count)],
                   m_ref, l_ref, acc_ref, rows, head, scale2, lim)

    def block(slot, count, masked):
        for head in range(heads):
            for r0 in range(0, n_rows, bm):
                unit(slot, count, masked, head, r0)

    def small_block(slot, masked):
        def per_head(head, carry):
            for r0 in range(0, n_rows, bm):
                unit(slot, 1, masked, head, r0)
            return carry
        lax.fori_loop(0, heads, per_head, 0)

    def body(i, carry):
        slot = lax.rem(i, 2)
        @pl.when(i + 1 < n_two)
        def _():
            for cp in copies(1 - slot, start + 2 * (i + 1), 2): cp.start()
        for cp in copies(slot, start + 2 * i, 2): cp.wait()
        block(slot, 2, False)
        return carry
    lax.fori_loop(0, n_two, body, 0)
    @pl.when(odd > 0)
    def _():
        for cp in copies(2, start + 2 * n_two, 1): cp.wait()
        small_block(2, False)
    @pl.when(limit > 0)
    def _():
        for cp in copies(3, tail, 1): cp.wait()
        small_block(3, True)


def flash(cache_len, q, kt, v, state, *, bm, mode, heads, n):
    n_rows, width = q.shape
    n_chunk, hd, ck = kt.shape
    vm = pl.BlockSpec(memory_space=pltpu.VMEM)
    anyspec = pl.BlockSpec(memory_space=pl.ANY)
    stat = (jax.ShapeDtypeStruct((n_rows, width), jnp.float32), jax.ShapeDtypeStruct((n_rows, heads * 128), jnp.float32),
            jax.ShapeDtypeStruct((n_rows, heads * 128), jnp.float32))
    kern = functools.partial(flash_kernel, bm=bm, mode=mode, heads=heads, n=n)
    first = mode == 'cache'
    if first:
        def kern(length, q, kt, v, *rest):
            flash_kernel(length, q, kt, v, None, None, None, *rest, bm=bm, mode=mode, heads=heads, n=n)
    ins = (cache_len, q, kt, v) + (() if first else tuple(state))
    return pl.pallas_call(
        kern, out_shape=stat,
        in_specs=[pl.BlockSpec(memory_space=pltpu.SMEM), vm, anyspec, anyspec] + ([] if first else [vm] * 3),
        out_specs=(vm,) * 3,
        scratch_shapes=[pltpu.VMEM((4, 2, hd, ck), jnp.bfloat16), pltpu.VMEM((4, 2, ck, hd), jnp.bfloat16),
                        pltpu.SemaphoreType.DMA((4, 4))],
        compiler_params=pltpu.CompilerParams(vmem_limit_bytes=48 * 1024 * 1024),
        input_output_aliases={} if first else {4: 0, 5: 1, 6: 2},
        cost_estimate=pl.CostEstimate(flops=2 * n_rows * width * n_chunk * ck, bytes_accessed=8 << 20,
                                      transcendentals=n_rows * heads * n_chunk * ck // 2),
        name=f"flash_{mode}",
    )(*ins)


def flip_kernel(*refs):
    half = len(refs) // 2
    for src, dst in zip(refs[:half], refs[half:]):
        dst[...] = src[...].T


def flip(*arrays):
    vm = pl.BlockSpec(memory_space=pltpu.VMEM)
    return pl.pallas_call(
        flip_kernel, out_shape=tuple(jax.ShapeDtypeStruct(a.shape[::-1], a.dtype) for a in arrays),
        in_specs=[vm] * len(arrays), out_specs=(vm,) * len(arrays),
        cost_estimate=pl.CostEstimate(flops=1 << 20, bytes_accessed=1 << 20, transcendentals=0), name="flip",
    )(*arrays)


def merge_kernel(acc_a, m_a, l_a, acc_b, m_b, l_b, o_ref, *, heads):
    hd = o_ref.shape[1] // heads
    scale2 = LOG2E * hd ** -0.5
    for head in range(heads):
        lanes = pl.ds(head * 128, 128)
        cols = pl.ds(head * hd, hd)
        top = jnp.maximum(m_a[:, lanes], m_b[:, lanes])
        w_a = jnp.exp2((m_a[:, lanes] - top) * scale2)
        w_b = jnp.exp2((m_b[:, lanes] - top) * scale2)
        den = jnp.sum(l_a[:, lanes] * w_a + l_b[:, lanes] * w_b, axis=1, keepdims=True)
        num = (acc_a[:, cols] * jnp.concatenate([w_a] * (hd // 128), axis=1)
               + acc_b[:, cols] * jnp.concatenate([w_b] * (hd // 128), axis=1))
        o_ref[:, cols] = (num / den).astype(jnp.bfloat16)


def merge(state_a, state_b, heads):
    n_rows, width = state_a[0].shape
    vm = pl.BlockSpec(memory_space=pltpu.VMEM)
    return pl.pallas_call(
        functools.partial(merge_kernel, heads=heads),
        out_shape=jax.ShapeDtypeStruct((n_rows, width), jnp.bfloat16),
        in_specs=[vm] * 6, out_specs=vm,
        compiler_params=pltpu.CompilerParams(vmem_limit_bytes=40 * 1024 * 1024),
        cost_estimate=pl.CostEstimate(flops=4 * n_rows * width, bytes_accessed=10 * n_rows * width, transcendentals=0),
        name="merge",
    )(*state_a, *state_b)


def band_kernel(first_ref, q_ref, kprev_ref, vprev_ref, kloc_ref, vloc_ref, kown_ref, vown_ref, o_ref, *, heads, bm):
    n_rows = q_ref.shape[0]
    hd = q_ref.shape[1] // heads
    scale2 = LOG2E * hd ** -0.5
    is_first = first_ref[0] > 0
    row = lax.broadcasted_iota(jnp.int32, (bm, bm), 0)
    col = lax.broadcasted_iota(jnp.int32, (bm, bm), 1)
    n_blk = n_rows // bm
    dims = (((1,), (1,)), ((), ()))

    def piece(prev_ref, loc_ref, own_ref, idx):
        if idx < n_blk:
            rows = pl.ds(idx * bm, bm)
            return jnp.where(is_first, loc_ref[rows, :], prev_ref[rows, :])
        return own_ref[pl.ds((idx - n_blk) * bm, bm), :]

    for blk in range(n_blk):
        keys = [piece(kprev_ref, kloc_ref, kown_ref, blk + i) for i in range(n_blk + 1)]
        vals = [piece(vprev_ref, vloc_ref, vown_ref, blk + i) for i in range(n_blk + 1)]
        for head in range(heads):
            cols = pl.ds(head * hd, hd)
            q = q_ref[pl.ds(blk * bm, bm), cols]
            scores = [lax.dot_general(q, k, dims, preferred_element_type=jnp.float32) for k in keys]
            scores[0] = jnp.where(col > row, scores[0], -jnp.inf)
            scores[-1] = jnp.where(col <= row, scores[-1], -jnp.inf)
            top = scores[0]
            for s in scores[1:]:
                top = jnp.maximum(top, s)
            top = jnp.max(top, axis=1, keepdims=True)
            total = None
            num = None
            for s, v in zip(scores, vals):
                e = jnp.exp2((s - top) * scale2)
                total = e if total is None else total + e
                term = jnp.dot(e.astype(jnp.bfloat16), v, preferred_element_type=jnp.float32)
                num = term if num is None else num + term
            o_ref[pl.ds(blk * bm, bm), cols] = (num / jnp.sum(total, axis=1, keepdims=True)).astype(jnp.bfloat16)


def band(first, q, kprev, vprev, kloc, vloc, kown, vown, heads, bm):
    vm = pl.BlockSpec(memory_space=pltpu.VMEM)
    n_rows, width = q.shape
    return pl.pallas_call(
        functools.partial(band_kernel, heads=heads, bm=bm),
        out_shape=jax.ShapeDtypeStruct((n_rows, width), jnp.bfloat16),
        in_specs=[pl.BlockSpec(memory_space=pltpu.SMEM)] + [vm] * 7, out_specs=vm,
        compiler_params=pltpu.CompilerParams(vmem_limit_bytes=40 * 1024 * 1024),
        cost_estimate=pl.CostEstimate(flops=8 * n_rows * width * n_rows, bytes_accessed=4 << 20, transcendentals=0),
        name="band",
    )(first, q, kprev, vprev, kloc, vloc, kown, vown)


def rms_norm(rows_in, gain_vec):
    rows_f32 = rows_in.astype(jnp.float32)
    inv_rms = lax.rsqrt(jnp.mean(rows_f32 * rows_f32, axis=-1, keepdims=True) + NORM_EPS)
    return (rows_f32 * inv_rms * gain_vec.astype(jnp.float32)).astype(jnp.bfloat16)


def project(rows_in, weight):
    return jnp.dot(rows_in, weight, preferred_element_type=jnp.float32).astype(jnp.bfloat16)


def add_residual(hidden, attn_out, w_out):
    return (hidden.astype(jnp.float32) + jnp.dot(attn_out, w_out, preferred_element_type=jnp.float32)).astype(jnp.bfloat16)


def mlp_block(hidden, gain_vec, w_gate, w_up, w_down):
    normed = rms_norm(hidden, gain_vec)
    gate_pre = jnp.dot(normed, w_gate, preferred_element_type=jnp.float32)
    up_pre = jnp.dot(normed, w_up, preferred_element_type=jnp.float32)
    act_bf16 = (jax.nn.gelu(gate_pre, approximate=True) * up_pre).astype(jnp.bfloat16)
    return (hidden.astype(jnp.float32) + jnp.dot(act_bf16, w_down, preferred_element_type=jnp.float32)).astype(jnp.bfloat16)


def solution(mesh):
    n = mesh.shape['ctx']
    holder = [d if d % 2 == 0 else n - d for d in range(n)]
    swap_pairs = [(d, holder[d]) for d in range(n)]
    halo_pairs = [(holder[c - 1], holder[c]) for c in range(1, n)]
    mate_pairs = [(d, d ^ 1) for d in range(n)]
    parity_groups = [[d for d in range(n) if d % 2 == p] for p in range(2)]
    row_spec = P(('dp', 'ctx'), None)
    cache_spec = P(None, ('dp', 'ctx'), None, None)
    local_spec = P(None, 'dp', None, None)
    in_specs = (row_spec, P('dp'), cache_spec, cache_spec, local_spec, local_spec) + (P(),) * 9

    def gather(x):
        return lax.all_gather(x, 'ctx', axis=0, axis_index_groups=parity_groups)

    def device_step(x_rows, cache_len, k_cache, v_cache, k_local, v_local, g_attn, g_mlp, w_q, w_k, w_v, w_o, w_gate, w_up, w_down):
        dev = lax.axis_index('ctx')
        par = lax.rem(dev, 2)
        chunk = jnp.where(par == 0, dev, n - dev)
        head_dim = k_local.shape[3]
        heads = w_q.shape[2] // head_dim
        pairs = k_cache.shape[0]
        first = jnp.where(chunk == 0, 1, 0).astype(jnp.int32).reshape(1)

        flipped = flip(*(k_cache[p, :, 0] for p in range(pairs)))
        caches = [(gather(flipped[p]), gather(v_cache[p, :, 0])) for p in range(pairs)]
        hidden = lax.ppermute(x_rows, 'ctx', swap_pairs)
        for pair in range(pairs):
            layer = 2 * pair
            normed = rms_norm(hidden, g_attn[layer])
            new_k, new_v = project(normed, w_k[layer]), project(normed, w_v[layer])
            halo = lax.ppermute(jnp.concatenate([new_k, new_v], axis=1), 'ctx', halo_pairs)
            q = project(normed, w_q[layer])
            out = band(first, q, halo[:, :head_dim], halo[:, head_dim:], k_local[pair, :, 0], v_local[pair, :, 0],
                       new_k, new_v, heads, BAND_ROWS)
            hidden = add_residual(hidden, out, w_o[layer])
            hidden = mlp_block(hidden, g_mlp[layer], w_gate[layer], w_up[layer], w_down[layer])

            layer = 2 * pair + 1
            normed = rms_norm(hidden, g_attn[layer])
            all_kt = gather(flip(project(normed, w_k[layer]))[0])
            all_v = gather(project(normed, w_v[layer]))
            q = project(normed, w_q[layer])
            mate_q = lax.ppermute(q, 'ctx', mate_pairs)
            args = dict(bm=FLASH_ROWS, heads=heads, n=n)
            own = flash(cache_len, q, *caches[pair], None, mode='cache', **args)
            mate = flash(cache_len, mate_q, *caches[pair], None, mode='cache', **args)
            own, mate = lax.optimization_barrier((own, mate))
            mate = flash(cache_len, mate_q, all_kt, all_v, mate, mode='mate', **args)
            back = [lax.ppermute(t, 'ctx', mate_pairs) for t in mate]
            own = flash(cache_len, q, all_kt, all_v, own, mode='own', **args)
            out = merge(own, back, heads)
            hidden = add_residual(hidden, out, w_o[layer])
            hidden = mlp_block(hidden, g_mlp[layer], w_gate[layer], w_up[layer], w_down[layer])
        return lax.ppermute(hidden, 'ctx', swap_pairs)

    return jax.shard_map(device_step, mesh=mesh, in_specs=in_specs, out_specs=row_spec, check_vma=False)
```

```python
import functools
import math
import jax, jax.numpy as jnp
from jax import lax
from jax.experimental import pallas as pl
from jax.experimental.pallas import tpu as pltpu
from jax.sharding import PartitionSpec as P

NORM_EPS = 1e-6
BAND_ROWS = 256
FF_BLOCKS = 4

LOG2E = 1.4426950408889634

NEG = -3.4028234663852886e38
STEPS = (((0, 0),), ((1, 0), (3, 0)), ((0, 1), (0, 3)), ((2, 0), (0, 2)), ((1, 1), (1, 3)), ((3, 1), (3, 3)),
         ((2, 1), (2, 3)), ((1, 2), (3, 2)), ((2, 2),))
SLOT = {off: (2 * j + 16) % 17 if i == 0 else 2 * j for j, offs in enumerate(STEPS) for i, off in enumerate(offs)}
N_STEP = len(STEPS)


def ring_kernel(len_ref, q_hbm, ktc_hbm, vc_hbm, ktn_hbm, vn_hbm,
                acc_own_ref, ml_own_ref, acc_mate_ref, ml_mate_ref,
                qs, acc_s, m_s, l_s, kbuf, vbuf, local_sem, send_sem, recv_sem, q_sem, *, n, side, heads, pair):
    n_rows = q_hbm.shape[0]
    hd = q_hbm.shape[1] // heads
    ck = kbuf.shape[3]
    scale2 = LOG2E * hd ** -0.5
    dev = lax.axis_index('ctx')
    par = lax.rem(dev, 2)
    chip = dev // 2
    x_pos = lax.rem(chip, side)
    y_pos = chip // side
    a_pos = x_pos * (1 - par) + y_pos * par
    b_pos = y_pos * (1 - par) + x_pos * par

    def device_at(a, b):
        a = lax.rem(a + side, side)
        b = lax.rem(b + side, side)
        x = a * (1 - par) + b * par
        y = b * (1 - par) + a * par
        return (y * side + x) * 2 + par

    peers = {'a+': device_at(a_pos + 1, b_pos), 'a-': device_at(a_pos - 1, b_pos),
             'b+': device_at(a_pos, b_pos + 1), 'b-': device_at(a_pos, b_pos - 1)}
    bufs = (kbuf, vbuf)
    sent = []

    def remote(number):
        phase, part, src, dst, peer = sent[number]
        return pltpu.make_async_remote_copy(
            src_ref=bufs[part].at[phase, SLOT[src]], dst_ref=bufs[part].at[phase, SLOT[dst]],
            send_sem=send_sem.at[number], recv_sem=recv_sem.at[phase, SLOT[dst], part],
            device_id={'ctx': peers[peer]}, device_id_type=pl.DeviceIdType.MESH)

    def send(phase, part, src, dst, peer):
        sent.append((phase, part, src, dst, peer))
        remote(len(sent) - 1).start()

    def arrived(phase, off, part):
        pltpu.make_async_remote_copy(
            src_ref=bufs[part].at[phase, SLOT[off]], dst_ref=bufs[part].at[phase, SLOT[off]],
            send_sem=send_sem.at[0], recv_sem=recv_sem.at[phase, SLOT[off], part],
            device_id={'ctx': peers['a+']}, device_id_type=pl.DeviceIdType.MESH).wait_recv()

    locals_ = [[pltpu.make_async_copy(src, bufs[part].at[phase, SLOT[(0, 0)]], local_sem.at[phase, part])
                for part, src in enumerate(srcs)] for phase, srcs in enumerate(((ktc_hbm.at[pair], vc_hbm.at[pair]), (ktn_hbm, vn_hbm)))]
    q_local = pltpu.make_async_copy(q_hbm, qs.at[0], q_sem.at[0])
    q_local.start()
    for copies in locals_:
        for cp in copies:
            cp.start()
    mate_dev = dev + 1 - 2 * par

    barrier = pltpu.get_barrier_semaphore()
    for peer in (*peers.values(), mate_dev):
        pl.semaphore_signal(barrier, inc=1, device_id={'ctx': peer}, device_id_type=pl.DeviceIdType.MESH)
    pl.semaphore_wait(barrier, 5)
    q_remote = pltpu.make_async_remote_copy(src_ref=q_hbm, dst_ref=qs.at[1], send_sem=q_sem.at[1], recv_sem=q_sem.at[2],
                                            device_id={'ctx': mate_dev}, device_id_type=pl.DeviceIdType.MESH)

    def start_own(phase):
        for cp in locals_[phase]:
            cp.wait()
        for part in range(2):
            for peer, dst in (('a+', (1, 0)), ('a-', (3, 0)), ('b+', (0, 1)), ('b-', (0, 3))):
                send(phase, part, (0, 0), dst, peer)

    def spread(phase, da, part):
        send(phase, part, (da, 0), (da, 1), 'b+')
        send(phase, part, (da, 0), (da, 3), 'b-')

    def comm(phase, step):
        if step == 1:
            arrived(phase, (1, 0), 0)
            send(phase, 0, (1, 0), (2, 0), 'a+')
            arrived(phase, (3, 0), 0)
            arrived(phase, (3, 0), 1)
            send(phase, 1, (3, 0), (2, 0), 'a-')
            arrived(phase, (1, 0), 1)
            for part in range(2):
                spread(phase, 1, part)
                spread(phase, 3, part)
        elif step == 3:
            for part in range(2):
                arrived(phase, (2, 0), part)
                spread(phase, 2, part)
            for part in range(2):
                arrived(phase, (0, 2), part)
        elif step in (2, 4, 5, 6):
            da = STEPS[step][0][0]
            for db, part in ((1, 0), (3, 1)):
                arrived(phase, (da, db), part)
                send(phase, part, (da, db), (da, 2), 'b+' if part == 0 else 'b-')
            for db, part in ((1, 1), (3, 0)):
                arrived(phase, (da, db), part)
        elif step in (7, 8):
            for off in STEPS[step]:
                for part in range(2):
                    arrived(phase, off, part)

    start_own(0)
    q_remote.start()
    m_s[...] = jnp.full(m_s.shape, NEG, jnp.float32)
    l_s[...] = jnp.zeros(l_s.shape, jnp.float32)
    acc_s[...] = jnp.zeros(acc_s.shape, jnp.float32)
    length = len_ref[0]
    q_local.wait()
    q_remote.wait()

    def attend(which, phase, slots, bias=None, causal=False):
        def scores(head):
            q = qs[which, :, pl.ds(head * hd, hd)]
            out = []
            for i, slot in enumerate(slots):
                s = jnp.dot(q, kbuf[phase, slot], preferred_element_type=jnp.float32)
                if bias is not None:
                    s = s + bias[i]
                if causal:
                    keep = lax.broadcasted_iota(jnp.int32, s.shape, 1) <= lax.broadcasted_iota(jnp.int32, s.shape, 0)
                    s = jnp.where(keep, s, -jnp.inf)
                out.append(s)
            return out

        def rest(head, s_list):
            lanes = pl.ds(head * 128, 128)
            parts = [s[:, i:i + 128] for s in s_list for i in range(0, ck, 128)]
            top = parts[0]
            for part in parts[1:]:
                top = jnp.maximum(top, part)
            m_old = m_s[which, :, lanes]
            m_new = jnp.maximum(m_old, jnp.max(top, axis=1, keepdims=True))
            alpha = jnp.exp2((m_old - m_new) * scale2)
            m_s[which, :, lanes] = m_new
            total = None
            probs = []
            for part in parts:
                e = jnp.exp2((part - m_new) * scale2)
                total = e if total is None else total + e
                probs.append(e.astype(jnp.bfloat16))
            l_s[which, :, lanes] = l_s[which, :, lanes] * alpha + total
            per = ck // 128
            num = None
            for i, slot in enumerate(slots):
                p = jnp.concatenate(probs[i * per:(i + 1) * per], axis=1)
                term = jnp.dot(p, vbuf[phase, slot], preferred_element_type=jnp.float32)
                num = term if num is None else num + term
            for c in range(0, hd, 128):
                cols = pl.ds(head * hd + c, 128)
                acc_s[which, :, cols] = acc_s[which, :, cols] * alpha + num[:, c:c + 128]

        ready = scores(0)
        for head in range(heads):
            now = ready
            if head + 1 < heads:
                ready = scores(head + 1)
            rest(head, now)

    col = lax.broadcasted_iota(jnp.int32, (1, ck), 1)

    def cache_bias(source):
        return jnp.where(col < length - source * ck, 0.0, -jnp.inf).astype(jnp.float32)

    def packed(i, j):
        return sum((offs[i][j] if i < len(offs) else 0) * side ** k for k, offs in enumerate(STEPS))

    digits = tuple(packed(i, j) for i in range(2) for j in range(2))

    def body(g, carry):
        phase = g // N_STEP
        step = lax.rem(g, N_STEP)
        da0, db0, da1, db1 = (lax.rem(c, side) for c in carry)
        for k in range(2 * N_STEP):
            if k % N_STEP > 0 or k == 0:
                if k == 0:
                    continue
                @pl.when(g == k)
                def _():
                    if k == 6:
                        start_own(1)
                    comm(k // N_STEP, k % N_STEP)
        slot0 = lax.rem(2 * step + 16, 17)
        slot1 = 2 * step
        src0 = device_at(a_pos - da0, b_pos - db0)
        src1 = device_at(a_pos - da1, b_pos - db1)
        paired = jnp.where(lax.rem(step, N_STEP - 1) == 0, 0, 1)

        @pl.when(phase == 0)
        def _():
            bias0, bias1 = cache_bias(src0), cache_bias(src1)

            def both(which, c):
                attend(which, 0, [slot0, slot1], [bias0, bias1])
                return c

            def one(which, c):
                attend(which, 0, [slot0], [bias0])
                return c

            @pl.when(paired == 1)
            def _():
                lax.fori_loop(0, 2, both, 0)

            @pl.when(paired == 0)
            def _():
                lax.fori_loop(0, 2, one, 0)

        @pl.when(phase == 1)
        def _():
            flip_ = n * par
            sign = 1 - 2 * par
            chunk0 = flip_ + sign * src0
            chunk1 = flip_ + sign * src1
            mine = flip_ + sign * dev
            mate = (n - dev - 1) * (1 - par) + (dev - 1) * par

            def new(which, c):
                q_chunk = mine * (1 - which) + mate * which
                use0 = jnp.where(chunk0 < q_chunk, 1, 0)
                use1 = jnp.where(chunk1 < q_chunk, 1, 0) * paired

                @pl.when(use0 + use1 == 2)
                def _():
                    attend(which, 1, [slot0, slot1])

                @pl.when(use0 + use1 == 1)
                def _():
                    attend(which, 1, [slot0 * use0 + slot1 * use1])
                return c
            lax.fori_loop(0, 2, new, 0)

            @pl.when(step == 0)
            def _():
                attend(0, 1, [SLOT[(0, 0)]], causal=True)
        return tuple(jnp.where(step == N_STEP - 1, d, c // side) for c, d in zip(carry, digits))

    lax.fori_loop(0, 2 * N_STEP, body, tuple(dev * 0 + d for d in digits))

    lane = lax.broadcasted_iota(jnp.int32, (n_rows, 128), 1)
    for which, (acc_ref, ml_ref) in enumerate(((acc_own_ref, ml_own_ref), (acc_mate_ref, ml_mate_ref))):
        acc_ref[...] = acc_s[which]
        ml = jnp.zeros((n_rows, 128), jnp.float32)
        for head in range(heads):
            lanes = pl.ds(head * 128, 128)
            ml = jnp.where(lane == head, m_s[which, :, lanes], ml)
            ml = jnp.where(lane == heads + head, jnp.sum(l_s[which, :, lanes], axis=1, keepdims=True), ml)
        ml_ref[...] = ml
    for number in range(len(sent)):
        remote(number).wait_send()


def ring(cache_len, q, kt_c, v_c, kt_n, v_n, *, n, heads, pair):
    n_rows, width = q.shape
    hd, ck = kt_n.shape
    side = math.isqrt(n // 2)
    assert 2 * side * side == n and side == 4
    vm = pl.BlockSpec(memory_space=pltpu.VMEM)
    anyspec = pl.BlockSpec(memory_space=pl.ANY)
    one = (jax.ShapeDtypeStruct((n_rows, width), jnp.float32), jax.ShapeDtypeStruct((n_rows, 128), jnp.float32))
    n_sent = 2 * 30
    return pl.pallas_call(
        functools.partial(ring_kernel, n=n, side=side, heads=heads, pair=pair),
        out_shape=one * 2,
        in_specs=[pl.BlockSpec(memory_space=pltpu.SMEM)] + [anyspec] * 5,
        out_specs=(vm,) * 4,
        scratch_shapes=[pltpu.VMEM((2, n_rows, width), jnp.bfloat16), pltpu.VMEM((2, n_rows, width), jnp.float32),
                        pltpu.VMEM((2, n_rows, heads * 128), jnp.float32), pltpu.VMEM((2, n_rows, heads * 128), jnp.float32),
                        pltpu.VMEM((2, 17, hd, ck), jnp.bfloat16), pltpu.VMEM((2, 17, ck, hd), jnp.bfloat16),
                        pltpu.SemaphoreType.DMA((2, 2)), pltpu.SemaphoreType.DMA((n_sent,)), pltpu.SemaphoreType.DMA((2, 17, 2)),
                        pltpu.SemaphoreType.DMA((3,))],
        compiler_params=pltpu.CompilerParams(vmem_limit_bytes=62 * 1024 * 1024, collective_id=pair, has_side_effects=True),
        cost_estimate=pl.CostEstimate(flops=6 * n_rows * width * n * ck, bytes_accessed=8 << 20,
                                      transcendentals=n_rows * heads * n * ck),
        name="ring",
    )(cache_len, q, kt_c, v_c, kt_n, v_n)


def flip_kernel(src, dst):
    for i in range(src.shape[0]):
        dst[i] = src[i].T


def flip(x):
    vm = pl.BlockSpec(memory_space=pltpu.VMEM)
    return pl.pallas_call(
        flip_kernel, out_shape=jax.ShapeDtypeStruct((x.shape[0], x.shape[2], x.shape[1]), x.dtype),
        in_specs=[vm], out_specs=vm,
        cost_estimate=pl.CostEstimate(flops=1 << 20, bytes_accessed=1 << 20, transcendentals=0), name="flip",
    )(x)


def band_kernel(q_ref, prev_ref, kloc_ref, vloc_ref, own_ref, o_ref, *, heads, bm, pair):
    n_rows = q_ref.shape[0]
    hd = q_ref.shape[1] // heads
    scale2 = LOG2E * hd ** -0.5
    is_first = lax.axis_index('ctx') == 0
    row = lax.broadcasted_iota(jnp.int32, (bm, bm), 0)
    col = lax.broadcasted_iota(jnp.int32, (bm, bm), 1)
    n_blk = n_rows // bm
    dims = (((1,), (1,)), ((), ()))

    def piece(loc_ref, lanes, idx):
        if idx < n_blk:
            rows = pl.ds(idx * bm, bm)
            return jnp.where(is_first, loc_ref[pair, rows, :], prev_ref[rows, lanes])
        return own_ref[pl.ds((idx - n_blk) * bm, bm), lanes]

    for blk in range(n_blk):
        keys = [piece(kloc_ref, pl.ds(0, hd), blk + i) for i in range(n_blk + 1)]
        vals = [piece(vloc_ref, pl.ds(hd, hd), blk + i) for i in range(n_blk + 1)]
        for head in range(heads):
            cols = pl.ds(head * hd, hd)
            q = q_ref[pl.ds(blk * bm, bm), cols]
            scores = [lax.dot_general(q, k, dims, preferred_element_type=jnp.float32) for k in keys]
            scores[0] = jnp.where(col > row, scores[0], -jnp.inf)
            scores[-1] = jnp.where(col <= row, scores[-1], -jnp.inf)
            top = scores[0]
            for s in scores[1:]:
                top = jnp.maximum(top, s)
            top = jnp.max(top, axis=1, keepdims=True)
            total = None
            num = None
            for s, v in zip(scores, vals):
                e = jnp.exp2((s - top) * scale2)
                total = e if total is None else total + e
                term = jnp.dot(e.astype(jnp.bfloat16), v, preferred_element_type=jnp.float32)
                num = term if num is None else num + term
            o_ref[pl.ds(blk * bm, bm), cols] = (num / jnp.sum(total, axis=1, keepdims=True)).astype(jnp.bfloat16)


def band(q, kv_prev, k_loc, v_loc, kv_own, *, heads, bm, pair):
    vm = pl.BlockSpec(memory_space=pltpu.VMEM)
    n_rows, width = q.shape
    return pl.pallas_call(
        functools.partial(band_kernel, heads=heads, bm=bm, pair=pair),
        out_shape=jax.ShapeDtypeStruct((n_rows, width), jnp.bfloat16),
        in_specs=[vm] * 5, out_specs=vm,
        compiler_params=pltpu.CompilerParams(vmem_limit_bytes=40 * 1024 * 1024),
        cost_estimate=pl.CostEstimate(flops=8 * n_rows * width * n_rows, bytes_accessed=4 << 20, transcendentals=0),
        name="band",
    )(q, kv_prev, k_loc, v_loc, kv_own)


def rms_norm(rows_in, gain_vec):
    rows_f32 = rows_in.astype(jnp.float32)
    inv_rms = lax.rsqrt(jnp.mean(rows_f32 * rows_f32, axis=-1, keepdims=True) + NORM_EPS)
    return (rows_f32 * inv_rms * gain_vec.astype(jnp.float32)).astype(jnp.bfloat16)


def qkv(x, layer, g_ref, wq_ref, wk_ref, wv_ref, outs, flip_k):
    h = rms_norm(x, g_ref[pl.ds(layer, 1), :])
    outs[0][...] = jnp.dot(h, wq_ref[...], preferred_element_type=jnp.float32).astype(jnp.bfloat16)
    k = jnp.dot(h, wk_ref[...], preferred_element_type=jnp.float32)
    v = jnp.dot(h, wv_ref[...], preferred_element_type=jnp.float32).astype(jnp.bfloat16)
    hd = v.shape[1]
    if flip_k:
        outs[1][...] = k.astype(jnp.bfloat16).T
        outs[2][...] = v
    else:
        outs[1][:, pl.ds(0, hd)] = k.astype(jnp.bfloat16)
        outs[1][:, pl.ds(hd, hd)] = v


def qkv_shapes(n_rows, width, hd, flip_k):
    tail = [(hd, n_rows), (n_rows, hd)] if flip_k else [(n_rows, 2 * hd)]
    return [jax.ShapeDtypeStruct(t, jnp.bfloat16) for t in [(n_rows, width)] + tail]


def enter(x, g_attn, w_q, w_k, w_v):
    def kernel(x_ref, g_ref, wq_ref, wk_ref, wv_ref, *outs):
        qkv(x_ref[...], 0, g_ref, wq_ref.at[0], wk_ref.at[0], wv_ref.at[0], outs, False)

    def first(w):
        return pl.BlockSpec((1,) + w.shape[1:], lambda i: (0, 0, 0))
    shapes = qkv_shapes(x.shape[0], w_q.shape[2], w_k.shape[2], False)
    full = lambda a: pl.BlockSpec(a.shape, lambda i: (0, 0))
    return pl.pallas_call(
        kernel, grid=(1,), out_shape=shapes,
        in_specs=[full(x), full(g_attn), first(w_q), first(w_k), first(w_v)],
        out_specs=[full(s) for s in shapes],
        compiler_params=pltpu.CompilerParams(vmem_limit_bytes=32 * 1024 * 1024),
        cost_estimate=pl.CostEstimate(flops=2 * x.shape[0] * x.shape[1] * 1536, bytes_accessed=4 << 20, transcendentals=0),
        name="enter",
    )(x, g_attn, w_q, w_k, w_v)


def leave_kernel(*refs, n_attn, layer, last, heads, flip_k):
    attn, refs = refs[:n_attn], refs[n_attn:]
    x_ref, gm_ref, wo_ref, wg_ref, wu_ref, wd_ref = refs[:6]
    refs = refs[6:]
    ga_ref, wq_ref, wk_ref, wv_ref = refs[:4] if not last else (None,) * 4
    refs = refs[0 if last else 4:]
    x_out, outs, (x_mid, h_mid, total) = refs[0], refs[1:-3], refs[-3:]
    step = pl.program_id(0)

    @pl.when(step == 0)
    def _():
        if n_attn == 1:
            o = attn[0][...]
        else:
            acc_a, ml_a, acc_b, ml_b = attn
            hd = acc_a.shape[1] // heads
            scale2 = LOG2E * hd ** -0.5
            pieces = []
            for head in range(heads):
                cols = pl.ds(head * hd, hd)
                m_a, m_b = ml_a[:, head:head + 1], ml_b[:, head:head + 1]
                l_a, l_b = ml_a[:, heads + head:heads + head + 1], ml_b[:, heads + head:heads + head + 1]
                top = jnp.maximum(m_a, m_b)
                w_a = jnp.exp2((m_a - top) * scale2)
                w_b = jnp.exp2((m_b - top) * scale2)
                den = l_a * w_a + l_b * w_b
                pieces.append(((acc_a[:, cols] * w_a + acc_b[:, cols] * w_b) / den).astype(jnp.bfloat16))
            o = jnp.concatenate(pieces, axis=1)
        x1 = (x_ref[...].astype(jnp.float32) + jnp.dot(o, wo_ref[0], preferred_element_type=jnp.float32)).astype(jnp.bfloat16)
        x_mid[...] = x1
        h_mid[...] = rms_norm(x1, gm_ref[pl.ds(layer, 1), :])
        total[...] = jnp.zeros_like(total)

    h = h_mid[...]
    gate = jnp.dot(h, wg_ref[0], preferred_element_type=jnp.float32)
    up = jnp.dot(h, wu_ref[0], preferred_element_type=jnp.float32)
    u = (jax.nn.gelu(gate, approximate=True) * up).astype(jnp.bfloat16)
    total[...] += jnp.dot(u, wd_ref[0], preferred_element_type=jnp.float32)

    @pl.when(step == pl.num_programs(0) - 1)
    def _():
        x2 = (x_mid[...].astype(jnp.float32) + total[...]).astype(jnp.bfloat16)
        x_out[...] = x2
        if not last:
            qkv(x2, layer + 1, ga_ref, wq_ref.at[0], wk_ref.at[0], wv_ref.at[0], outs, flip_k)


def leave(attn, x, layer, g_attn, g_mlp, w_q, w_k, w_v, w_o, w_gate, w_up, w_down, *, heads, last):
    n_rows, d = x.shape
    ff = w_gate.shape[2]
    n_blk = FF_BLOCKS
    flip_k = layer % 2 == 0
    full = lambda a: pl.BlockSpec(a.shape, lambda i: (0,) * len(a.shape))
    at = lambda w, l: pl.BlockSpec((1,) + w.shape[1:], lambda i: (l, 0, 0))
    wide = pl.BlockSpec((1, d, ff // n_blk), lambda i: (layer, 0, i))
    ins = list(attn) + [x, g_mlp, w_o, w_gate, w_up, w_down]
    specs = [full(a) for a in attn] + [full(x), full(g_mlp), at(w_o, layer), wide, wide, pl.BlockSpec((1, ff // n_blk, d), lambda i: (layer, i, 0))]
    shapes = [jax.ShapeDtypeStruct(x.shape, x.dtype)]
    if not last:
        ins += [g_attn, w_q, w_k, w_v]
        specs += [full(g_attn), at(w_q, layer + 1), at(w_k, layer + 1), at(w_v, layer + 1)]
        shapes += qkv_shapes(n_rows, w_q.shape[2], w_k.shape[2], flip_k)
    return pl.pallas_call(
        functools.partial(leave_kernel, n_attn=len(attn), layer=layer, last=last, heads=heads, flip_k=flip_k),
        grid=(n_blk,), out_shape=shapes, in_specs=specs, out_specs=[full(s) for s in shapes],
        scratch_shapes=[pltpu.VMEM((n_rows, d), jnp.bfloat16), pltpu.VMEM((n_rows, d), jnp.bfloat16), pltpu.VMEM((n_rows, d), jnp.float32)],
        compiler_params=pltpu.CompilerParams(vmem_limit_bytes=56 * 1024 * 1024, dimension_semantics=("arbitrary",)),
        cost_estimate=pl.CostEstimate(flops=2 * n_rows * d * (3 * ff + 2560), bytes_accessed=14 << 20, transcendentals=n_rows * ff),
        name="leave",
    )(*ins)


def solution(mesh):
    n = mesh.shape['ctx']
    holder = [d if d % 2 == 0 else n - d for d in range(n)]
    swap_pairs = [(d, holder[d]) for d in range(n)]
    halo_pairs = [(holder[c - 1], holder[c]) for c in range(1, n)]
    mate_pairs = [(d, d ^ 1) for d in range(n)]
    row_spec = P(('dp', 'ctx'), None)
    cache_spec = P(None, ('dp', 'ctx'), None, None)
    local_spec = P(None, 'dp', None, None)
    in_specs = (row_spec, P('dp'), cache_spec, cache_spec, local_spec, local_spec) + (P(),) * 9

    def device_step(x_rows, cache_len, k_cache, v_cache, k_local, v_local, g_attn, g_mlp, w_q, w_k, w_v, w_o, w_gate, w_up, w_down):
        head_dim = k_local.shape[3]
        heads = w_q.shape[2] // head_dim
        k_cache, v_cache, k_local, v_local = (t.reshape(t.shape[0], t.shape[1], head_dim) for t in (k_cache, v_cache, k_local, v_local))
        pairs = k_cache.shape[0]
        cache_kt = flip(k_cache)
        hidden = lax.ppermute(x_rows, 'ctx', swap_pairs)
        q, kv = enter(hidden, g_attn, w_q, w_k, w_v)

        def after(attn, x, layer):
            return leave(attn, x, layer, g_attn, g_mlp, w_q, w_k, w_v, w_o, w_gate, w_up, w_down,
                         heads=heads, last=layer == 2 * pairs - 1)

        for pair in range(pairs):
            out = band(q, lax.ppermute(kv, 'ctx', halo_pairs), k_local, v_local, kv, heads=heads, bm=BAND_ROWS, pair=pair)
            hidden, q, new_kt, new_v = after([out], hidden, 2 * pair)
            acc, ml, mate_acc, mate_ml = ring(cache_len, q, cache_kt, v_cache, new_kt, new_v, n=n, heads=heads, pair=pair)
            back = [lax.ppermute(t, 'ctx', mate_pairs) for t in (mate_acc, mate_ml)]
            hidden, *rest = after([acc, ml] + back, hidden, 2 * pair + 1)
            if rest:
                q, kv = rest
        return lax.ppermute(hidden, 'ctx', swap_pairs)

    return jax.shard_map(device_step, mesh=mesh, in_specs=in_specs, out_specs=row_spec, check_vma=False)
```

```python
import functools
import math
import jax, jax.numpy as jnp
from jax import lax
from jax.experimental import pallas as pl
from jax.experimental.pallas import tpu as pltpu
from jax.sharding import PartitionSpec as P

NORM_EPS = 1e-6
BAND_ROWS = 256
FF_BLOCKS = 4
VMEM_BYTES = 62 * 1024 * 1024

LOG2E = 1.4426950408889634

NEG = -3.4028234663852886e38
STEPS = (((0, 0),), ((1, 0), (3, 0)), ((0, 1), (0, 3)), ((2, 0), (0, 2)), ((1, 1), (1, 3)), ((3, 1), (3, 3)),
         ((2, 1), (2, 3)), ((1, 2), (3, 2)), ((2, 2),))
SLOT = {off: (2 * j + 16) % 17 if i == 0 else 2 * j for j, offs in enumerate(STEPS) for i, off in enumerate(offs)}
N_STEP = len(STEPS)
EVENTS = ((), ((0, 1), (0, 2)), ((0, 3),), ((0, 4),), ((1, 0), (0, 5)), ((0, 6),), ((1, 1), (0, 7)), ((0, 8), (1, 2)), ((1, 3),),
          ((1, 4),), ((1, 5),), ((1, 6),), ((1, 7),), ((1, 8),))


def ring_kernel(len_ref, q_hbm, ktc_hbm, vc_hbm, ktn_hbm, vn_hbm,
                acc_own_ref, ml_own_ref, acc_mate_ref, ml_mate_ref,
                qs, acc_s, m_s, l_s, kbuf, vbuf, local_sem, send_sem, recv_sem, q_sem, *, n, side, heads, pair):
    n_rows = q_hbm.shape[0]
    hd = q_hbm.shape[1] // heads
    ck = kbuf.shape[3]
    scale2 = LOG2E * hd ** -0.5
    dev = lax.axis_index('ctx')
    par = lax.rem(dev, 2)
    chip = dev // 2
    x_pos = lax.rem(chip, side)
    y_pos = chip // side
    a_pos = x_pos * (1 - par) + y_pos * par
    b_pos = y_pos * (1 - par) + x_pos * par

    def device_at(a, b):
        a = lax.rem(a + side, side)
        b = lax.rem(b + side, side)
        x = a * (1 - par) + b * par
        y = b * (1 - par) + a * par
        return (y * side + x) * 2 + par

    peers = {'a+': device_at(a_pos + 1, b_pos), 'a-': device_at(a_pos - 1, b_pos),
             'b+': device_at(a_pos, b_pos + 1), 'b-': device_at(a_pos, b_pos - 1)}
    bufs = (kbuf, vbuf)
    sent = []

    def remote(number):
        phase, part, src, dst, peer = sent[number]
        return pltpu.make_async_remote_copy(
            src_ref=bufs[part].at[phase, SLOT[src]], dst_ref=bufs[part].at[phase, SLOT[dst]],
            send_sem=send_sem.at[number], recv_sem=recv_sem.at[phase, SLOT[dst], part],
            device_id={'ctx': peers[peer]}, device_id_type=pl.DeviceIdType.MESH)

    def send(phase, part, src, dst, peer):
        sent.append((phase, part, src, dst, peer))
        remote(len(sent) - 1).start()

    def arrived(phase, off, part):
        pltpu.make_async_remote_copy(
            src_ref=bufs[part].at[phase, SLOT[off]], dst_ref=bufs[part].at[phase, SLOT[off]],
            send_sem=send_sem.at[0], recv_sem=recv_sem.at[phase, SLOT[off], part],
            device_id={'ctx': peers['a+']}, device_id_type=pl.DeviceIdType.MESH).wait_recv()

    locals_ = [[pltpu.make_async_copy(src, bufs[part].at[phase, SLOT[(0, 0)]], local_sem.at[phase, part])
                for part, src in enumerate(srcs)] for phase, srcs in enumerate(((ktc_hbm.at[pair], vc_hbm.at[pair]), (ktn_hbm, vn_hbm)))]
    q_local = pltpu.make_async_copy(q_hbm, qs.at[0], q_sem.at[0])
    q_local.start()
    for copies in locals_:
        for cp in copies:
            cp.start()
    mate_dev = dev + 1 - 2 * par

    barrier = pltpu.get_barrier_semaphore()
    for peer in (*peers.values(), mate_dev):
        pl.semaphore_signal(barrier, inc=1, device_id={'ctx': peer}, device_id_type=pl.DeviceIdType.MESH)
    pl.semaphore_wait(barrier, 5)
    q_remote = pltpu.make_async_remote_copy(src_ref=q_hbm, dst_ref=qs.at[1], send_sem=q_sem.at[1], recv_sem=q_sem.at[2],
                                            device_id={'ctx': mate_dev}, device_id_type=pl.DeviceIdType.MESH)

    def start_own(phase):
        for cp in locals_[phase]:
            cp.wait()
        for part in range(2):
            for peer, dst in (('a+', (1, 0)), ('a-', (3, 0)), ('b+', (0, 1)), ('b-', (0, 3))):
                send(phase, part, (0, 0), dst, peer)

    def spread(phase, da, part):
        send(phase, part, (da, 0), (da, 1), 'b+')
        send(phase, part, (da, 0), (da, 3), 'b-')

    def comm(phase, step):
        if step == 1:
            arrived(phase, (1, 0), 0)
            send(phase, 0, (1, 0), (2, 0), 'a+')
            arrived(phase, (3, 0), 0)
            arrived(phase, (3, 0), 1)
            send(phase, 1, (3, 0), (2, 0), 'a-')
            arrived(phase, (1, 0), 1)
            for part in range(2):
                spread(phase, 1, part)
                spread(phase, 3, part)
        elif step == 3:
            for part in range(2):
                arrived(phase, (2, 0), part)
                spread(phase, 2, part)
            for part in range(2):
                arrived(phase, (0, 2), part)
        elif step in (2, 4, 5, 6):
            da = STEPS[step][0][0]
            for db, part in ((1, 0), (3, 1)):
                arrived(phase, (da, db), part)
                send(phase, part, (da, db), (da, 2), 'b+' if part == 0 else 'b-')
            for db, part in ((1, 1), (3, 0)):
                arrived(phase, (da, db), part)
        elif step in (7, 8):
            for off in STEPS[step]:
                for part in range(2):
                    arrived(phase, off, part)

    start_own(0)
    q_remote.start()
    m_s[...] = jnp.full(m_s.shape, NEG, jnp.float32)
    l_s[...] = jnp.zeros(l_s.shape, jnp.float32)
    acc_s[...] = jnp.zeros(acc_s.shape, jnp.float32)
    length = len_ref[0]
    q_local.wait()
    q_remote.wait()

    def attend(which, phase, slots, bias=None, causal=False):
        def scores(head):
            q = qs[which, :, pl.ds(head * hd, hd)]
            out = []
            for i, slot in enumerate(slots):
                s = jnp.dot(q, kbuf[phase, slot], preferred_element_type=jnp.float32)
                if bias is not None:
                    s = s + bias[i]
                if causal:
                    keep = lax.broadcasted_iota(jnp.int32, s.shape, 1) <= lax.broadcasted_iota(jnp.int32, s.shape, 0)
                    s = jnp.where(keep, s, -jnp.inf)
                out.append(s)
            return out

        def rest(head, s_list):
            lanes = pl.ds(head * 128, 128)
            parts = [s[:, i:i + 128] for s in s_list for i in range(0, ck, 128)]
            top = parts[0]
            for part in parts[1:]:
                top = jnp.maximum(top, part)
            m_old = m_s[which, :, lanes]
            m_new = jnp.maximum(m_old, jnp.max(top, axis=1, keepdims=True))
            alpha = jnp.exp2((m_old - m_new) * scale2)
            m_s[which, :, lanes] = m_new
            total = None
            probs = []
            for part in parts:
                e = jnp.exp2((part - m_new) * scale2)
                total = e if total is None else total + e
                probs.append(e.astype(jnp.bfloat16))
            l_s[which, :, lanes] = l_s[which, :, lanes] * alpha + total
            per = ck // 128
            num = None
            for i, slot in enumerate(slots):
                p = jnp.concatenate(probs[i * per:(i + 1) * per], axis=1)
                term = jnp.dot(p, vbuf[phase, slot], preferred_element_type=jnp.float32)
                num = term if num is None else num + term
            for c in range(0, hd, 128):
                cols = pl.ds(head * hd + c, 128)
                acc_s[which, :, cols] = acc_s[which, :, cols] * alpha + num[:, c:c + 128]

        ready = scores(0)
        for head in range(heads):
            now = ready
            if head + 1 < heads:
                ready = scores(head + 1)
            rest(head, now)

    col = lax.broadcasted_iota(jnp.int32, (1, ck), 1)

    def cache_bias(source):
        return jnp.where(col < length - source * ck, 0.0, -jnp.inf).astype(jnp.float32)

    def packed(i, j):
        return sum((offs[i][j] if i < len(offs) else 0) * side ** k for k, offs in enumerate(STEPS))

    digits = tuple(packed(i, j) for i in range(2) for j in range(2))

    def body(g, carry):
        phase = g // N_STEP
        step = lax.rem(g, N_STEP)
        da0, db0, da1, db1 = (lax.rem(c, side) for c in carry)
        for k, events in enumerate(EVENTS):
            if events:
                @pl.when(g == k)
                def _():
                    for event in events:
                        if event[1] == 0:
                            start_own(event[0])
                        else:
                            comm(*event)
        slot0 = lax.rem(2 * step + 16, 17)
        slot1 = 2 * step
        src0 = device_at(a_pos - da0, b_pos - db0)
        src1 = device_at(a_pos - da1, b_pos - db1)
        paired = jnp.where(lax.rem(step, N_STEP - 1) == 0, 0, 1)

        @pl.when(phase == 0)
        def _():
            bias0, bias1 = cache_bias(src0), cache_bias(src1)

            def both(which, c):
                attend(which, 0, [slot0, slot1], [bias0, bias1])
                return c

            def one(which, c):
                attend(which, 0, [slot0], [bias0])
                return c

            @pl.when(paired == 1)
            def _():
                lax.fori_loop(0, 2, both, 0)

            @pl.when(paired == 0)
            def _():
                lax.fori_loop(0, 2, one, 0)

        @pl.when(phase == 1)
        def _():
            def new(which, c):
                q_chunk = dev * (1 - which) + mate_dev * which
                use0 = jnp.where(src0 < q_chunk, 1, 0)
                use1 = jnp.where(src1 < q_chunk, 1, 0) * paired

                @pl.when(use0 + use1 == 2)
                def _():
                    attend(which, 1, [slot0, slot1])

                @pl.when(use0 + use1 == 1)
                def _():
                    attend(which, 1, [slot0 * use0 + slot1 * use1])
                return c
            lax.fori_loop(0, 2, new, 0)

            @pl.when(step == 0)
            def _():
                attend(0, 1, [SLOT[(0, 0)]], causal=True)
        return tuple(jnp.where(step == N_STEP - 1, d, c // side) for c, d in zip(carry, digits))

    lax.fori_loop(0, 2 * N_STEP, body, tuple(dev * 0 + d for d in digits))

    lane = lax.broadcasted_iota(jnp.int32, (n_rows, 128), 1)
    for which, (acc_ref, ml_ref) in enumerate(((acc_own_ref, ml_own_ref), (acc_mate_ref, ml_mate_ref))):
        acc_ref[...] = acc_s[which]
        ml = jnp.zeros((n_rows, 128), jnp.float32)
        for head in range(heads):
            lanes = pl.ds(head * 128, 128)
            ml = jnp.where(lane == head, m_s[which, :, lanes], ml)
            ml = jnp.where(lane == heads + head, jnp.sum(l_s[which, :, lanes], axis=1, keepdims=True), ml)
        ml_ref[...] = ml
    for number in range(len(sent)):
        remote(number).wait_send()


def ring(cache_len, q, kt_c, v_c, kt_n, v_n, *, n, heads, pair):
    n_rows, width = q.shape
    hd, ck = kt_n.shape
    side = math.isqrt(n // 2)
    assert 2 * side * side == n and side == 4
    vm = pl.BlockSpec(memory_space=pltpu.VMEM)
    anyspec = pl.BlockSpec(memory_space=pl.ANY)
    one = (jax.ShapeDtypeStruct((n_rows, width), jnp.float32), jax.ShapeDtypeStruct((n_rows, 128), jnp.float32))
    n_sent = 2 * 30
    return pl.pallas_call(
        functools.partial(ring_kernel, n=n, side=side, heads=heads, pair=pair),
        out_shape=one * 2,
        in_specs=[pl.BlockSpec(memory_space=pltpu.SMEM)] + [anyspec] * 5,
        out_specs=(vm,) * 4,
        scratch_shapes=[pltpu.VMEM((2, n_rows, width), jnp.bfloat16), pltpu.VMEM((2, n_rows, width), jnp.float32),
                        pltpu.VMEM((2, n_rows, heads * 128), jnp.float32), pltpu.VMEM((2, n_rows, heads * 128), jnp.float32),
                        pltpu.VMEM((2, 17, hd, ck), jnp.bfloat16), pltpu.VMEM((2, 17, ck, hd), jnp.bfloat16),
                        pltpu.SemaphoreType.DMA((2, 2)), pltpu.SemaphoreType.DMA((n_sent,)), pltpu.SemaphoreType.DMA((2, 17, 2)),
                        pltpu.SemaphoreType.DMA((3,))],
        compiler_params=pltpu.CompilerParams(vmem_limit_bytes=VMEM_BYTES, collective_id=pair, has_side_effects=True),
        cost_estimate=pl.CostEstimate(flops=6 * n_rows * width * n * ck, bytes_accessed=8 << 20,
                                      transcendentals=n_rows * heads * n * ck),
        name="ring",
    )(cache_len, q, kt_c, v_c, kt_n, v_n)


def flip_kernel(src, dst):
    for i in range(src.shape[0]):
        dst[i] = src[i].T


def flip(x):
    vm = pl.BlockSpec(memory_space=pltpu.VMEM)
    return pl.pallas_call(
        flip_kernel, out_shape=jax.ShapeDtypeStruct((x.shape[0], x.shape[2], x.shape[1]), x.dtype),
        in_specs=[vm], out_specs=vm, compiler_params=pltpu.CompilerParams(vmem_limit_bytes=VMEM_BYTES),
        cost_estimate=pl.CostEstimate(flops=1 << 20, bytes_accessed=1 << 20, transcendentals=0), name="flip",
    )(x)


def band_kernel(q_ref, prev_ref, kloc_ref, vloc_ref, own_ref, o_ref, *, heads, bm, pair):
    n_rows = q_ref.shape[0]
    hd = q_ref.shape[1] // heads
    scale2 = LOG2E * hd ** -0.5
    is_first = lax.axis_index('ctx') == 0
    row = lax.broadcasted_iota(jnp.int32, (bm, bm), 0)
    col = lax.broadcasted_iota(jnp.int32, (bm, bm), 1)
    n_blk = n_rows // bm
    dims = (((1,), (1,)), ((), ()))

    def piece(loc_ref, lanes, idx):
        if idx < n_blk:
            rows = pl.ds(idx * bm, bm)
            return jnp.where(is_first, loc_ref[pair, rows, :], prev_ref[rows, lanes])
        return own_ref[pl.ds((idx - n_blk) * bm, bm), lanes]

    for blk in range(n_blk):
        keys = [piece(kloc_ref, pl.ds(0, hd), blk + i) for i in range(n_blk + 1)]
        vals = [piece(vloc_ref, pl.ds(hd, hd), blk + i) for i in range(n_blk + 1)]
        for head in range(heads):
            cols = pl.ds(head * hd, hd)
            q = q_ref[pl.ds(blk * bm, bm), cols]
            scores = [lax.dot_general(q, k, dims, preferred_element_type=jnp.float32) for k in keys]
            scores[0] = jnp.where(col > row, scores[0], -jnp.inf)
            scores[-1] = jnp.where(col <= row, scores[-1], -jnp.inf)
            top = scores[0]
            for s in scores[1:]:
                top = jnp.maximum(top, s)
            top = jnp.max(top, axis=1, keepdims=True)
            total = None
            num = None
            for s, v in zip(scores, vals):
                e = jnp.exp2((s - top) * scale2)
                total = e if total is None else total + e
                term = jnp.dot(e.astype(jnp.bfloat16), v, preferred_element_type=jnp.float32)
                num = term if num is None else num + term
            o_ref[pl.ds(blk * bm, bm), cols] = (num / jnp.sum(total, axis=1, keepdims=True)).astype(jnp.bfloat16)


def band(q, kv_prev, k_loc, v_loc, kv_own, *, heads, bm, pair):
    vm = pl.BlockSpec(memory_space=pltpu.VMEM)
    n_rows, width = q.shape
    return pl.pallas_call(
        functools.partial(band_kernel, heads=heads, bm=bm, pair=pair),
        out_shape=jax.ShapeDtypeStruct((n_rows, width), jnp.bfloat16),
        in_specs=[vm] * 5, out_specs=vm,
        compiler_params=pltpu.CompilerParams(vmem_limit_bytes=VMEM_BYTES),
        cost_estimate=pl.CostEstimate(flops=8 * n_rows * width * n_rows, bytes_accessed=4 << 20, transcendentals=0),
        name="band",
    )(q, kv_prev, k_loc, v_loc, kv_own)


def rms_norm(rows_in, gain_vec):
    rows_f32 = rows_in.astype(jnp.float32)
    inv_rms = lax.rsqrt(jnp.mean(rows_f32 * rows_f32, axis=-1, keepdims=True) + NORM_EPS)
    return (rows_f32 * inv_rms * gain_vec.astype(jnp.float32)).astype(jnp.bfloat16)


def qkv(x, layer, g_ref, wq_ref, wk_ref, wv_ref, outs, flip_k):
    h = rms_norm(x, g_ref[pl.ds(layer, 1), :])
    outs[0][...] = jnp.dot(h, wq_ref[...], preferred_element_type=jnp.float32).astype(jnp.bfloat16)
    k = jnp.dot(h, wk_ref[...], preferred_element_type=jnp.float32)
    v = jnp.dot(h, wv_ref[...], preferred_element_type=jnp.float32).astype(jnp.bfloat16)
    hd = v.shape[1]
    if flip_k:
        outs[1][...] = k.astype(jnp.bfloat16).T
        outs[2][...] = v
    else:
        outs[1][:, pl.ds(0, hd)] = k.astype(jnp.bfloat16)
        outs[1][:, pl.ds(hd, hd)] = v


def qkv_shapes(n_rows, width, hd, flip_k):
    tail = [(hd, n_rows), (n_rows, hd)] if flip_k else [(n_rows, 2 * hd)]
    return [jax.ShapeDtypeStruct(t, jnp.bfloat16) for t in [(n_rows, width)] + tail]


def enter(x, g_attn, w_q, w_k, w_v):
    def kernel(x_ref, g_ref, wq_ref, wk_ref, wv_ref, *outs):
        qkv(x_ref[...], 0, g_ref, wq_ref.at[0], wk_ref.at[0], wv_ref.at[0], outs, False)

    def first(w):
        return pl.BlockSpec((1,) + w.shape[1:], lambda i: (0, 0, 0))
    shapes = qkv_shapes(x.shape[0], w_q.shape[2], w_k.shape[2], False)
    full = lambda a: pl.BlockSpec(a.shape, lambda i: (0, 0))
    return pl.pallas_call(
        kernel, grid=(1,), out_shape=shapes,
        in_specs=[full(x), full(g_attn), first(w_q), first(w_k), first(w_v)],
        out_specs=[full(s) for s in shapes],
        compiler_params=pltpu.CompilerParams(vmem_limit_bytes=VMEM_BYTES),
        cost_estimate=pl.CostEstimate(flops=2 * x.shape[0] * x.shape[1] * 1536, bytes_accessed=4 << 20, transcendentals=0),
        name="enter",
    )(x, g_attn, w_q, w_k, w_v)


def leave_kernel(*refs, n_attn, layer, last, heads, flip_k):
    attn, refs = refs[:n_attn], refs[n_attn:]
    x_ref, gm_ref, wo_hbm, wg_hbm, wu_hbm, wd_hbm = refs[:6]
    refs = refs[6:]
    ga_ref, wq_hbm, wk_hbm, wv_hbm = refs[:4] if not last else (None,) * 4
    refs = refs[0 if last else 4:]
    n_scratch = 6 if last else 9
    x_out, outs = refs[0], refs[1:-n_scratch]
    wo, wg, wu, wd, total, sems, *proj = refs[-n_scratch:]
    n_blk, _, blk = wg.shape

    def block_copies(j):
        cols = pl.ds(pl.multiple_of(j * blk, blk), blk)
        return (pltpu.make_async_copy(wg_hbm.at[layer, :, cols], wg.at[j], sems.at[j, 0]),
                pltpu.make_async_copy(wu_hbm.at[layer, :, cols], wu.at[j], sems.at[j, 1]),
                pltpu.make_async_copy(wd_hbm.at[layer, cols, :], wd.at[j], sems.at[j, 2]))

    copy_o = pltpu.make_async_copy(wo_hbm.at[layer], wo, sems.at[n_blk, 0])
    copy_o.start()
    for j in range(n_blk):
        for cp in block_copies(j):
            cp.start()
    tail = [] if last else [pltpu.make_async_copy(src.at[layer + 1], dst, sems.at[n_blk + 1, i])
                            for i, (src, dst) in enumerate(zip((wq_hbm, wk_hbm, wv_hbm), proj))]
    for cp in tail:
        cp.start()

    if n_attn == 1:
        o = attn[0][...]
    else:
        acc_a, ml_a, acc_b, ml_b = attn
        hd = acc_a.shape[1] // heads
        scale2 = LOG2E * hd ** -0.5
        pieces = []
        for head in range(heads):
            cols = pl.ds(head * hd, hd)
            m_a, m_b = ml_a[:, head:head + 1], ml_b[:, head:head + 1]
            l_a, l_b = ml_a[:, heads + head:heads + head + 1], ml_b[:, heads + head:heads + head + 1]
            top = jnp.maximum(m_a, m_b)
            w_a = jnp.exp2((m_a - top) * scale2)
            w_b = jnp.exp2((m_b - top) * scale2)
            den = l_a * w_a + l_b * w_b
            pieces.append(((acc_a[:, cols] * w_a + acc_b[:, cols] * w_b) / den).astype(jnp.bfloat16))
        o = jnp.concatenate(pieces, axis=1)
    copy_o.wait()
    x1 = (x_ref[...].astype(jnp.float32) + jnp.dot(o, wo[...], preferred_element_type=jnp.float32)).astype(jnp.bfloat16)
    x_out[...] = x1
    h = rms_norm(x1, gm_ref[pl.ds(layer, 1), :])
    total[...] = jnp.zeros_like(total)

    def block(j, carry):
        for cp in block_copies(j):
            cp.wait()
        gate = jnp.dot(h, wg[j], preferred_element_type=jnp.float32)
        up = jnp.dot(h, wu[j], preferred_element_type=jnp.float32)
        u = (jax.nn.gelu(gate, approximate=True) * up).astype(jnp.bfloat16)
        total[...] += jnp.dot(u, wd[j], preferred_element_type=jnp.float32)
        return carry
    lax.fori_loop(0, n_blk, block, 0)

    x2 = (x_out[...].astype(jnp.float32) + total[...]).astype(jnp.bfloat16)
    x_out[...] = x2
    for cp in tail:
        cp.wait()
    if not last:
        qkv(x2, layer + 1, ga_ref, *proj, outs, flip_k)


def leave(attn, x, layer, g_attn, g_mlp, w_q, w_k, w_v, w_o, w_gate, w_up, w_down, *, heads, last):
    n_rows, d = x.shape
    ff = w_gate.shape[2]
    blk = ff // FF_BLOCKS
    flip_k = layer % 2 == 0
    vm = pl.BlockSpec(memory_space=pltpu.VMEM)
    anyspec = pl.BlockSpec(memory_space=pl.ANY)
    ins = list(attn) + [x, g_mlp, w_o, w_gate, w_up, w_down]
    specs = [vm] * (len(attn) + 2) + [anyspec] * 4
    shapes = [jax.ShapeDtypeStruct(x.shape, x.dtype)]
    scratch = [pltpu.VMEM(w_o.shape[1:], w_o.dtype), pltpu.VMEM((FF_BLOCKS, d, blk), x.dtype), pltpu.VMEM((FF_BLOCKS, d, blk), x.dtype),
               pltpu.VMEM((FF_BLOCKS, blk, d), x.dtype), pltpu.VMEM((n_rows, d), jnp.float32), pltpu.SemaphoreType.DMA((FF_BLOCKS + 2, 3))]
    if not last:
        ins += [g_attn, w_q, w_k, w_v]
        specs += [vm] + [anyspec] * 3
        shapes += qkv_shapes(n_rows, w_q.shape[2], w_k.shape[2], flip_k)
        scratch += [pltpu.VMEM(w.shape[1:], w.dtype) for w in (w_q, w_k, w_v)]
    return pl.pallas_call(
        functools.partial(leave_kernel, n_attn=len(attn), layer=layer, last=last, heads=heads, flip_k=flip_k),
        out_shape=shapes, in_specs=specs, out_specs=[vm] * len(shapes), scratch_shapes=scratch,
        compiler_params=pltpu.CompilerParams(vmem_limit_bytes=VMEM_BYTES),
        cost_estimate=pl.CostEstimate(flops=2 * n_rows * d * (3 * ff + 2560), bytes_accessed=14 << 20, transcendentals=n_rows * ff),
        name="leave",
    )(*ins)


def solution(mesh):
    n = mesh.shape['ctx']
    halo_pairs = [(d - 1, d) for d in range(1, n)]
    mate_pairs = [(d, d ^ 1) for d in range(n)]
    row_spec = P(('dp', 'ctx'), None)
    cache_spec = P(None, ('dp', 'ctx'), None, None)
    local_spec = P(None, 'dp', None, None)
    in_specs = (row_spec, P('dp'), cache_spec, cache_spec, local_spec, local_spec) + (P(),) * 9

    def device_step(x_rows, cache_len, k_cache, v_cache, k_local, v_local, g_attn, g_mlp, w_q, w_k, w_v, w_o, w_gate, w_up, w_down):
        head_dim = k_local.shape[3]
        heads = w_q.shape[2] // head_dim
        k_cache, v_cache, k_local, v_local = (t.reshape(t.shape[0], t.shape[1], head_dim) for t in (k_cache, v_cache, k_local, v_local))
        pairs = k_cache.shape[0]
        cache_kt = flip(k_cache)
        hidden = x_rows
        q, kv = enter(hidden, g_attn, w_q, w_k, w_v)

        def after(attn, x, layer):
            return leave(attn, x, layer, g_attn, g_mlp, w_q, w_k, w_v, w_o, w_gate, w_up, w_down,
                         heads=heads, last=layer == 2 * pairs - 1)

        for pair in range(pairs):
            out = band(q, lax.ppermute(kv, 'ctx', halo_pairs), k_local, v_local, kv, heads=heads, bm=BAND_ROWS, pair=pair)
            hidden, q, new_kt, new_v = after([out], hidden, 2 * pair)
            acc, ml, mate_acc, mate_ml = ring(cache_len, q, cache_kt, v_cache, new_kt, new_v, n=n, heads=heads, pair=pair)
            back = [lax.ppermute(t, 'ctx', mate_pairs) for t in (mate_acc, mate_ml)]
            hidden, *rest = after([acc, ml] + back, hidden, 2 * pair + 1)
            if rest:
                q, kv = rest
        return hidden

    return jax.shard_map(device_step, mesh=mesh, in_specs=in_specs, out_specs=row_spec, check_vma=False)
```
